128 devices in a mesh: ens: 8 (over x, core), dp: 16 (over y, z).
Axes of the slice: x: 4, y: 4, z: 4, core: 2. Of those that a mesh axis runs over, the one named last changes fastest.
Arguments:
- features: bfloat16 [6144, 256], P('dp'), may hold values from -4 to 4
- reward: float32 [6144], P('dp'), may hold values from -16 to 16
- done: int32 [6144], P('dp'), may hold values 0 or 1
- value_next: float32 [6144], P('dp'), may hold values from -16 to 16
- value_now: float32 [6144], P('dp'), may hold values from -4 to 4
- w_in: bfloat16 [16, 256, 2048], P('ens'), may hold values from -0.375 to 0.375
- w_mid: bfloat16 [16, 2048, 2048], P('ens'), may hold values from -0.099121094 to 0.099121094
- biases: float32 [2, 16, 2048], P(None, 'ens'), may hold values from -3 to 3
- w_out: bfloat16 [16, 2048], P('ens'), may hold values from -0.011048543 to 0.011048543
Outputs:
- value_grad: float32 [6144], P('dp')
- d_in: float32 [256, 16, 2048], P('dp', 'ens')
- d_mid: float32 [2048, 16, 2048], P('dp', 'ens')
- d_bias: float32 [2, 16, 2048], P(None, 'ens', 'dp')
- d_out: float32 [16, 2048], P('ens', 'dp')
The draws below stay inside these ranges and needn't reach their ends.
All inputs are finite; a program needn't handle non-finite values. No bound on the sum of `done` on one device may be relied on, other than what follows from the above.
Results may differ from the reference program's by a relative error of at most 0.013.
Values may be sent and summed in bfloat16 or wider, within the bound.
A program may use at most 128 MiB of HBM per device.

```python
import jax
import jax.numpy as jnp
from jax import lax

IN = 256
H = 2048
ROWS_DEV = 384
HEADS = 16
TOTAL = 6144


def draw_w_out(key, part):
    sign_key = jax.random.fold_in(key, 11)
    scale_key = jax.random.fold_in(key, 12)
    sign_values = (2 * jax.random.randint(sign_key, (HEADS, H), 0, 2) - 1).astype(jnp.float32)
    lowest = 0.5
    magnitude = jax.random.uniform(scale_key, (HEADS, H), jnp.float32, lowest, 1.0)
    return (sign_values * magnitude * (0.5 * H ** (-0.5))).astype(jnp.bfloat16)


def plant(entries, own_key, least, top_value):
    longest = entries.shape.index(max(entries.shape))
    spots = []
    for shift in (0, 1):
        where = [jax.random.randint(jax.random.fold_in(own_key, axis), (), 0, length) for axis, length in enumerate(entries.shape)]
        where[longest] = (where[longest] + shift) % entries.shape[longest]
        spots.append(tuple(where))
    return entries.at[spots[0]].set(least).at[spots[1]].set(top_value)


def steps_of(rng, extent, cuts, low, top_value):
    loudness = 1.0
    for dim, shards_of in cuts:
        heights = jax.random.uniform(jax.random.fold_in(jax.random.fold_in(rng, 6), dim), (shards_of,), jnp.float32, low / len(cuts), top_value / len(cuts))
        loudness = loudness * jnp.repeat(jnp.exp(heights), extent[dim] // shards_of).reshape((-1,) + (1,) * (len(extent) - 1 - dim))
    return loudness


def gaussian(stream_key, extent, scale, limit, shards=(), dtype=jnp.bfloat16):
    result = scale * jax.random.normal(stream_key, extent, jnp.float32)
    if shards:
        result = result * steps_of(stream_key, extent, shards, -0.22, 0.18)
    return jnp.clip(result, -limit, limit).astype(dtype)


def setup_inputs(seed: int = 0) -> dict:
    arg_keys = jax.random.split(jax.random.key(seed), 10)
    return {
        "features": jnp.clip(jax.random.uniform(arg_keys[0], (TOTAL, IN), jnp.float32, -4.0, 4.0) * steps_of(arg_keys[0], (TOTAL, IN), ((0, 16),), -0.4, 0.0), -4.0, 4.0).astype(jnp.bfloat16),
        "reward": gaussian(arg_keys[1], (TOTAL,), 4.0, 16.0, ((0, 16),), jnp.float32),
        "done": plant((jax.random.randint(arg_keys[2], (TOTAL,), 0, 10) < 1).astype(jnp.int32), jax.random.fold_in(arg_keys[2], 1), 0, 1),
        "value_next": gaussian(arg_keys[3], (TOTAL,), 4.0, 16.0, ((0, 16),), jnp.float32),
        "value_now": gaussian(arg_keys[4], (TOTAL,), 0.5, 4.0, ((0, 16),), jnp.float32),
        "w_in": gaussian(arg_keys[5], (HEADS, IN, H), IN ** -0.5, 0.375, ((0, 8),)),
        "w_mid": jnp.clip(jax.random.uniform(arg_keys[6], (HEADS, H, H), jnp.float32, -0.099121094, 0.099121094) * steps_of(arg_keys[6], (HEADS, H, H), ((0, 8),), -0.4, 0.0), -0.099121094, 0.099121094).astype(jnp.bfloat16),
        "biases": gaussian(arg_keys[7], (2, HEADS, H), 0.5, 3.0, ((1, 8),), jnp.float32),
        "w_out": draw_w_out(jax.random.fold_in(arg_keys[9], 71), 0),
    }


def silu_slope(value):
    sig = jax.nn.sigmoid(value)
    return sig * (1.0 + value * (1.0 - sig))


def rounded(value):
    return lax.optimization_barrier(value.astype(jnp.bfloat16)).astype(jnp.float32)


def reference(features, reward, done, value_next, value_now, w_in, w_mid, biases, w_out):
    total = features.shape[0]
    blocks = total // ROWS_DEV
    width_in = features.shape[1]
    hidden = w_mid.shape[1]
    feat_blocks = features.reshape(blocks, ROWS_DEV, width_in)
    target = reward + 0.99 * (1.0 - done.astype(jnp.float32)) * value_next
    target_blocks = target.reshape(blocks, ROWS_DEV)
    high = lax.Precision.HIGHEST

    def head_pass(params):
        w_first, w_second, bias_pair, w_last = params

        def step(carry, blk):
            xrows, trow = blk
            pre_one = jnp.dot(xrows, w_first, preferred_element_type=jnp.float32) + bias_pair[0]
            act_one = jax.nn.silu(pre_one).astype(jnp.bfloat16)
            pre_two = jnp.dot(act_one, w_second, preferred_element_type=jnp.float32) + bias_pair[1]
            act_two = jax.nn.silu(pre_two).astype(jnp.bfloat16)
            q_row = jnp.dot(act_two.astype(jnp.float32), w_last.astype(jnp.float32), precision=high)
            error = q_row - trow
            delta_two = (error[:, None] * w_last.astype(jnp.float32)[None, :] * silu_slope(pre_two)).astype(jnp.bfloat16)
            back = jnp.dot(delta_two, w_second.T, preferred_element_type=jnp.float32)
            delta_one = (back * silu_slope(pre_one)).astype(jnp.bfloat16)
            part_in = jnp.dot(xrows.T, delta_one, preferred_element_type=jnp.float32)
            part_mid = jnp.dot(act_one.T, delta_two, preferred_element_type=jnp.float32)
            part_bias = jnp.stack([jnp.sum(delta_one.astype(jnp.float32), axis=0), jnp.sum(delta_two.astype(jnp.float32), axis=0)])
            part_out = jnp.dot(error, act_two.astype(jnp.float32), precision=high)
            sums = (carry[0] + rounded(part_in), carry[1] + rounded(part_mid), carry[2] + rounded(part_bias), carry[3] + rounded(part_out))
            return sums, q_row

        start = (jnp.zeros((width_in, hidden), jnp.float32), jnp.zeros((hidden, hidden), jnp.float32),
                 jnp.zeros((2, hidden), jnp.float32), jnp.zeros((hidden,), jnp.float32))
        sums, q_rows = lax.scan(step, start, (feat_blocks, target_blocks))
        return sums[0], sums[1], sums[2], sums[3], q_rows.reshape(total)

    grad_in, grad_mid, grad_bias, grad_out, q_values = lax.map(
        head_pass, (w_in, w_mid, jnp.transpose(biases, (1, 0, 2)), w_out))
    q_min = jnp.min(q_values, axis=0)
    gap = q_min - value_now
    weight = jnp.where(gap < 0.0, 0.3, 0.7)
    value_grad = -2.0 * weight * gap
    return (value_grad, jnp.transpose(grad_in, (1, 0, 2)), jnp.transpose(grad_mid, (1, 0, 2)),
            jnp.transpose(grad_bias, (1, 0, 2)), grad_out)
```

```python
import jax
import jax.numpy as jnp
from jax import lax
from jax.experimental import pallas as pl
from jax.experimental.pallas import tpu as pltpu
from jax.sharding import PartitionSpec as P

MESH = pl.DeviceIdType.MESH
BF = jnp.bfloat16
F32 = jnp.float32
ROWS = 384
IN = 256
H = 2048
R2 = 2 * ROWS
C = 256
NC = H // C
GW = H + 256
HALF = H // 2
GH = GW // 2


def tn(a, b, **kw):
    return lax.dot_general(a, b, (((1,), (0,)), ((), ())), preferred_element_type=F32, **kw)


def nt(a, b, **kw):
    return lax.dot_general(a, b, (((1,), (1,)), ((), ())), preferred_element_type=F32, **kw)


def chunk(n, width=C):
    return pl.ds(pl.multiple_of(n * width, width), width)


def kernel(
    feat_hbm, reward, done, vnext, vnow, win_hbm, wmid_hbm, biases, wout,
    vg_out, mid_out, gin_out,
    feat, win, wmid, act1, sl1, act2, sl2, del2, accq, eb, stats, part, lhs, featT,
    r1a, r1b, r2a, r2b, r3, gp, g1a, g1b, g2a, g2b, g3,
    tgt, tgtm, qm, qr, mo, ms, mm, mx,
    lsem, wsem, osem, ssem, rsem,
):
    ens = lax.axis_index("ens")
    dp = lax.axis_index("dp")
    core = lax.rem(ens, 2)
    xpos = lax.div(ens, 2)
    y = lax.div(dp, 4)
    z = lax.rem(dp, 4)
    u = jnp.where(core == 0, y, z)
    v = jnp.where(core == 0, z, y)
    su = 4 - 3 * core
    sv = 1 + 3 * core
    head = lax.div(v, 2)

    def dp_of(ru, rv):
        return (u ^ ru) * su + (v ^ rv) * sv

    def dev(ru, rv):
        return (ens, dp_of(ru, rv))

    u1, u3, v1, v3 = dev(1, 0), dev(3, 0), dev(0, 1), dev(0, 3)
    sib = (ens ^ 1, dp)
    xs = [((xpos ^ k) * 2 + core, dp) for k in (1, 2, 3)]

    loads = [
        pltpu.make_async_copy(feat_hbm, feat.at[pl.ds(0, ROWS)], lsem.at[0]),
        pltpu.make_async_copy(win_hbm.at[head], win, lsem.at[1]),
    ]
    for n in range(NC):
        loads.append(
            pltpu.make_async_copy(
                wmid_hbm.at[head, :, pl.ds(n * C, C)], wmid.at[:, pl.ds(n * C, C)], wsem.at[n]
            )
        )
    for copy in loads:
        copy.start()

    barrier = pltpu.get_barrier_semaphore()
    partners = [u1, u3, v1, v3, sib, *xs]
    for p in partners:
        pl.semaphore_signal(barrier, inc=1, device_id=p, device_id_type=MESH)

    target = reward[...] + 0.99 * (1.0 - done[...].astype(F32)) * vnext[...]
    tgt[...] = jnp.broadcast_to(target, (8, ROWS))
    pl.semaphore_wait(barrier, len(partners))

    copies = []

    def send(src, dst, to):
        i = len(copies)
        copy = pltpu.make_async_remote_copy(
            src_ref=src, dst_ref=dst, send_sem=ssem.at[i], recv_sem=rsem.at[i],
            device_id=to, device_id_type=MESH,
        )
        copies.append(copy)
        copy.start()
        return copy

    loads[0].wait()
    got_feat = send(feat.at[pl.ds(0, ROWS)], feat.at[pl.ds(ROWS, ROWS)], v3)
    got_tgt = send(tgt, tgtm, v3)
    loads[1].wait()

    wo = wout[...].astype(F32)
    wo = jnp.where(head == 0, wo[0:1], wo[1:2])
    b_all = biases[...]
    b_one = jnp.where(head == 0, b_all[0, 0:1], b_all[0, 1:2])
    b_two = jnp.where(head == 0, b_all[1, 0:1], b_all[1, 1:2])
    stats[...] = jnp.zeros_like(stats)
    stats[0:1, :] = b_one
    stats[1:2, :] = b_two
    stats[2:3, :] = wo

    def silu_both(val):
        s = 0.5 * jnp.tanh(0.5 * val) + 0.5
        act = val * s
        return act, s + act * (1.0 - s)

    for p in range(2):
        rows = pl.ds(p * ROWS, ROWS)
        if p == 1:
            got_feat.wait_recv()

        @pl.loop(0, NC)
        def _(n):
            cols = chunk(n)
            val = tn(feat[rows, :], win[:, cols]) + stats[0:1, cols]
            act, slope = silu_both(val)
            act1[rows, cols] = act.astype(BF)
            sl1[rows, cols] = slope.astype(BF)

        accq[rows, :] = jnp.zeros((ROWS, 128), F32)
        if p == 0:
            for copy in loads[2:]:
                copy.wait()

        @pl.loop(0, NC)
        def _(n):
            cols = chunk(n)
            val = tn(act1[rows, :], wmid[:, cols]) + stats[1:2, cols]
            act, slope = silu_both(val)
            wrow = stats[2:3, cols]
            prod = act * wrow
            accq[rows, :] += prod[:, :128] + prod[:, 128:]
            act2[rows, cols] = act.astype(BF)
            sl2[rows, cols] = (slope * wrow).astype(BF)

    q = nt(jnp.ones((8, 128), F32), accq[...], precision=lax.Precision.HIGHEST)
    got_tgt.wait_recv()
    qm[...] = q[:, ROWS:]
    mo[...] = q[:, :ROWS]
    got_q = send(qm, qr, v3)
    err = q - jnp.concatenate([tgt[...], tgtm[...]], axis=1)
    eb[...] = jnp.transpose(jnp.broadcast_to(err[0:1], (128, R2)))
    stats[...] = jnp.zeros_like(stats)

    @pl.loop(0, NC)
    def _(n):
        cols = chunk(n)
        e = jnp.concatenate([eb[...], eb[...]], axis=1)
        d = e * sl2[:, cols].astype(F32)
        del2[:, cols] = d.astype(BF)
        stats[1:2, cols] = jnp.sum(d, axis=0, keepdims=True)
        stats[2:3, cols] = jnp.sum(e * act2[:, cols].astype(F32), axis=0, keepdims=True)

    order = (2, 1, 3, 0)

    def group(ru):
        for rv in range(4):
            lhs[pl.ds(rv * 128, 128), :] = jnp.transpose(act1[:, chunk(dp_of(ru, rv), 128)])

    def products(ru, half):
        @pl.loop(half * NC // 2, (half + 1) * NC // 2)
        def _(n):
            cols = chunk(n)
            res = tn(lhs[...], del2[:, cols]).astype(BF)
            for rv in range(4):
                part[ru, rv, :, cols] = res[rv * 128 : (rv + 1) * 128]

    left, right = pl.ds(0, HALF), pl.ds(HALF, HALF)
    one_a, one_b, two_a, two_b = [None] * 4, [None] * 4, [None] * 4, [None] * 4
    group(2)
    products(2, 0)
    for rv in order:
        one_a[rv] = send(part.at[2, rv, :, left], r1a.at[rv], u1)
    products(2, 1)
    for rv in order:
        one_b[rv] = send(part.at[2, rv, :, right], r1b.at[rv], u3)
    group(1)
    products(1, 0)
    for rv in order:
        two_a[rv] = [send(part.at[1, rv, :, left], r2a.at[rv, :, left], u1)]
    products(1, 1)
    group(3)
    products(3, 1)
    for rv in order:
        two_b[rv] = [send(part.at[3, rv, :, right], r2b.at[rv, :, right], u3)]
    products(3, 0)
    group(0)
    products(0, 0)
    products(0, 1)

    got_q.wait_recv()
    mo[...] = jnp.minimum(mo[...], qr[...])
    got_sib = send(mo, ms, sib)

    def merge():
        for rv in order:
            one_a[rv].wait_recv()
            part[3, rv, :, left] = (part[3, rv, :, left].astype(F32) + r1a[rv].astype(F32)).astype(BF)
            two_b[rv].append(send(part.at[3, rv, :, left], r2b.at[rv, :, left], u3))
            one_b[rv].wait_recv()
            part[1, rv, :, right] = (part[1, rv, :, right].astype(F32) + r1b[rv].astype(F32)).astype(BF)
            two_a[rv].append(send(part.at[1, rv, :, right], r2a.at[rv, :, right], u1))

    featT[...] = jnp.transpose(feat[...])

    @pl.loop(0, NC)
    def _(n):
        cols = chunk(n)
        back = nt(del2[...], wmid[cols, :])
        d = back * sl1[:, cols].astype(F32)
        stats[0:1, cols] = jnp.sum(d, axis=0, keepdims=True)
        res = tn(featT[...], d.astype(BF)).astype(BF)
        for i in range(16):
            slot = jnp.where(core == 0, (i // 4 ^ y) * 4 + (i % 4 ^ z), (i % 4 ^ z) * 4 + (i // 4 ^ y))
            gp[slot, :, cols] = res[i * 16 : (i + 1) * 16]

    for i in range(16):
        slot = jnp.where(core == 0, (i // 4 ^ y) * 4 + (i % 4 ^ z), (i % 4 ^ z) * 4 + (i // 4 ^ y))
        tile = jnp.concatenate([stats[:, i * 128 : (i + 1) * 128], jnp.zeros((8, 128), F32)], axis=0)
        gp[slot, :, pl.ds(H, 128)] = tile.astype(BF)
        gp[slot, :, pl.ds(H + 128, 128)] = jnp.zeros((16, 128), BF)

    got_sib.wait_recv()
    mm[...] = jnp.minimum(mo[...], ms[...])
    got_x = [send(mm, mx.at[k], xs[k]) for k in range(3)]

    gl, gr = pl.ds(0, GH), pl.ds(GH, GH)
    g_one_a = send(gp.at[pl.ds(8, 4), :, gl], g1a, u1)
    g_one_b = send(gp.at[pl.ds(8, 4), :, gr], g1b, u3)
    g_two_a = [send(gp.at[pl.ds(4, 4), :, gl], g2a.at[:, :, gl], u1)]
    g_two_b = [send(gp.at[pl.ds(12, 4), :, gr], g2b.at[:, :, gr], u3)]

    merge()

    g_one_a.wait_recv()
    gp[12:16, :, gl] = (gp[12:16, :, gl].astype(F32) + g1a[...].astype(F32)).astype(BF)
    g_two_b.append(send(gp.at[pl.ds(12, 4), :, gl], g2b.at[:, :, gl], u3))
    g_one_b.wait_recv()
    gp[4:8, :, gr] = (gp[4:8, :, gr].astype(F32) + g1b[...].astype(F32)).astype(BF)
    g_two_a.append(send(gp.at[pl.ds(4, 4), :, gr], g2a.at[:, :, gr], u1))

    def ring_sum(rv):
        for copy in (*two_a[rv], *two_b[rv]):
            copy.wait_recv()
        part[0, rv] = (part[0, rv].astype(F32) + r2a[rv].astype(F32) + r2b[rv].astype(F32)).astype(BF)

    ring_sum(2)
    three_3 = send(part.at[0, 2], r3.at[1], v1)
    ring_sum(1)
    three_0 = send(part.at[0, 1], r3.at[0], v1)
    ring_sum(3)
    three_3.wait_recv()
    part[0, 3] = (part[0, 3].astype(F32) + r3[1].astype(F32)).astype(BF)
    four = send(part.at[0, 3], mid_out.at[head], v3)

    for copy in (*g_two_a, *g_two_b):
        copy.wait_recv()
    gp[0:4] = (gp[0:4].astype(F32) + g2a[...].astype(F32) + g2b[...].astype(F32)).astype(BF)
    g_three = send(gp.at[pl.ds(1, 2)], g3, v1)

    ring_sum(0)
    three_0.wait_recv()
    part[0, 0] = (part[0, 0].astype(F32) + r3[0].astype(F32)).astype(BF)
    own_mid = pltpu.make_async_copy(part.at[0, 0], mid_out.at[head], osem.at[0])
    own_mid.start()

    g_three.wait_recv()
    gp[3] = (gp[3].astype(F32) + g3[1].astype(F32)).astype(BF)
    g_four = send(gp.at[3], gin_out.at[head], v3)
    gp[0] = (gp[0].astype(F32) + g3[0].astype(F32)).astype(BF)
    own_gin = pltpu.make_async_copy(gp.at[0], gin_out.at[head], osem.at[1])
    own_gin.start()

    for copy in got_x:
        copy.wait_recv()
    q_min = jnp.minimum(jnp.minimum(mm[...], mx[0]), jnp.minimum(mx[1], mx[2]))
    gap = q_min[0:1] - vnow[...]
    vg_out[...] = -2.0 * jnp.where(gap < 0.0, 0.3, 0.7) * gap

    own_mid.wait()
    own_gin.wait()
    four.wait_recv()
    g_four.wait_recv()
    for copy in copies:
        copy.wait_send()


def per_device(features, reward, done, value_next, value_now, w_in, w_mid, biases, w_out):
    vm = pl.BlockSpec(memory_space=pltpu.VMEM)
    hbm = pl.BlockSpec(memory_space=pl.ANY)
    line = (1, ROWS)
    vg, mid, gin = pl.pallas_call(
        kernel,
        out_shape=(
            jax.ShapeDtypeStruct(line, F32),
            jax.ShapeDtypeStruct((2, 128, H), BF),
            jax.ShapeDtypeStruct((2, 16, GW), BF),
        ),
        in_specs=[hbm, vm, vm, vm, vm, hbm, hbm, vm, vm],
        out_specs=(vm, hbm, hbm),
        scratch_shapes=[
            pltpu.VMEM((R2, IN), BF),
            pltpu.VMEM((IN, H), BF),
            pltpu.VMEM((H, H), BF),
            pltpu.VMEM((R2, H), BF),
            pltpu.VMEM((R2, H), BF),
            pltpu.VMEM((R2, H), BF),
            pltpu.VMEM((R2, H), BF),
            pltpu.VMEM((R2, H), BF),
            pltpu.VMEM((R2, 128), F32),
            pltpu.VMEM((R2, 128), F32),
            pltpu.VMEM((8, H), F32),
            pltpu.VMEM((4, 4, 128, H), BF),
            pltpu.VMEM((512, R2), BF),
            pltpu.VMEM((IN, R2), BF),
            pltpu.VMEM((4, 128, HALF), BF),
            pltpu.VMEM((4, 128, HALF), BF),
            pltpu.VMEM((4, 128, H), BF),
            pltpu.VMEM((4, 128, H), BF),
            pltpu.VMEM((2, 128, H), BF),
            pltpu.VMEM((16, 16, GW), BF),
            pltpu.VMEM((4, 16, GH), BF),
            pltpu.VMEM((4, 16, GH), BF),
            pltpu.VMEM((4, 16, GW), BF),
            pltpu.VMEM((4, 16, GW), BF),
            pltpu.VMEM((2, 16, GW), BF),
            *[pltpu.VMEM((8, ROWS), F32)] * 7,
            pltpu.VMEM((3, 8, ROWS), F32),
            pltpu.SemaphoreType.DMA((2,)),
            pltpu.SemaphoreType.DMA((NC,)),
            pltpu.SemaphoreType.DMA((2,)),
            pltpu.SemaphoreType.DMA((48,)),
            pltpu.SemaphoreType.DMA((48,)),
        ],
        compiler_params=pltpu.CompilerParams(
            collective_id=0, has_side_effects=True, vmem_limit_bytes=67_000_000
        ),
    )(
        features, reward.reshape(line), done.reshape(line), value_next.reshape(line),
        value_now.reshape(line), w_in, w_mid, biases, w_out,
    )
    d_mid = jnp.transpose(mid, (1, 0, 2)).astype(F32)
    d_in = jnp.transpose(gin[:, :, :H], (1, 0, 2)).astype(F32)
    rest = gin[:, :3, H : H + 128].astype(F32)
    d_bias = jnp.transpose(rest[:, :2], (1, 0, 2))
    return vg.reshape(ROWS), d_in, d_mid, d_bias, rest[:, 2]


def solution(mesh):
    in_specs = (
        P("dp", None), P("dp"), P("dp"), P("dp"), P("dp"),
        P("ens", None, None), P("ens", None, None), P(None, "ens", None), P("ens", None),
    )
    out_specs = (
        P("dp"), P("dp", "ens", None), P("dp", "ens", None), P(None, "ens", "dp"), P("ens", "dp"),
    )
    return jax.shard_map(
        per_device, mesh=mesh, in_specs=in_specs, out_specs=out_specs, check_vma=False
    )
```

```python
import jax
import jax.numpy as jnp
from jax import lax
from jax.experimental import pallas as pl
from jax.experimental.pallas import tpu as pltpu
from jax.sharding import PartitionSpec as P

MESH = pl.DeviceIdType.MESH
BF = jnp.bfloat16
F32 = jnp.float32
ROWS = 384
IN = 256
H = 2048
R2 = 2 * ROWS
C = 256
NC = H // C
C1 = 512
C2 = 512
C3 = 512
C5 = 512
GW = H + 256
HALF = H // 2
GH = GW // 2


def tn(a, b, **kw):
    return lax.dot_general(a, b, (((1,), (0,)), ((), ())), preferred_element_type=F32, **kw)


def nt(a, b, **kw):
    return lax.dot_general(a, b, (((1,), (1,)), ((), ())), preferred_element_type=F32, **kw)


def chunk(n, width=C):
    return pl.ds(pl.multiple_of(n * width, width), width)


def kernel(
    feat_hbm, reward, done, vnext, vnow, win_hbm, wmid_hbm, biases, wout,
    vg_out, mid_out, gin_out,
    feat, win, wmid, act1, sl1, act2, sl2, del2, accq, eb, stats, part, lhs, featT,
    r1a, r1b, r2a, r2b, r3, gp, g1a, g1b, g2a, g2b, g3,
    tgt, tgtm, qm, qr, mo, ms, mm, mx,
    lsem, wsem, osem, ssem, rsem,
):
    ens = lax.axis_index("ens")
    dp = lax.axis_index("dp")
    core = lax.rem(ens, 2)
    xpos = lax.div(ens, 2)
    y = lax.div(dp, 4)
    z = lax.rem(dp, 4)
    u = jnp.where(core == 0, y, z)
    v = jnp.where(core == 0, z, y)
    su = 4 - 3 * core
    sv = 1 + 3 * core
    head = lax.div(v, 2)

    def dp_of(ru, rv):
        return (u ^ ru) * su + (v ^ rv) * sv

    def dev(ru, rv):
        return (ens, dp_of(ru, rv))

    u1, u3, v1, v3 = dev(1, 0), dev(3, 0), dev(0, 1), dev(0, 3)
    sib = (ens ^ 1, dp)
    xs = [((xpos ^ k) * 2 + core, dp) for k in (1, 2, 3)]

    loads = [
        pltpu.make_async_copy(feat_hbm, feat.at[pl.ds(0, ROWS)], lsem.at[0]),
        pltpu.make_async_copy(win_hbm.at[head], win, lsem.at[1]),
    ]
    for n in range(NC):
        loads.append(
            pltpu.make_async_copy(
                wmid_hbm.at[head, :, pl.ds(n * C, C)], wmid.at[:, pl.ds(n * C, C)], wsem.at[n]
            )
        )
    for copy in loads:
        copy.start()

    barrier = pltpu.get_barrier_semaphore()
    partners = [u1, u3, v1, v3, sib, *xs]
    for p in partners:
        pl.semaphore_signal(barrier, inc=1, device_id=p, device_id_type=MESH)

    target = reward[...] + 0.99 * (1.0 - done[...].astype(F32)) * vnext[...]
    tgt[...] = jnp.broadcast_to(target.reshape(1, ROWS), (8, ROWS))
    pl.semaphore_wait(barrier, len(partners))

    copies = []

    def send(src, dst, to):
        i = len(copies)
        copy = pltpu.make_async_remote_copy(
            src_ref=src, dst_ref=dst, send_sem=ssem.at[i], recv_sem=rsem.at[i],
            device_id=to, device_id_type=MESH,
        )
        copies.append(copy)
        copy.start()
        return copy

    loads[0].wait()
    got_feat = send(feat.at[pl.ds(0, ROWS)], feat.at[pl.ds(ROWS, ROWS)], v3)
    got_tgt = send(tgt, tgtm, v3)
    loads[1].wait()

    wo = wout[...].astype(F32)
    wo = jnp.where(head == 0, wo[0:1], wo[1:2])
    b_all = biases[...]
    b_one = jnp.where(head == 0, b_all[0, 0:1], b_all[0, 1:2])
    b_two = jnp.where(head == 0, b_all[1, 0:1], b_all[1, 1:2])
    stats[...] = jnp.zeros_like(stats)
    stats[0:1, :] = b_one
    stats[1:2, :] = b_two
    stats[2:3, :] = wo

    def silu_both(val):
        s = 0.5 * jnp.tanh(0.5 * val) + 0.5
        act = val * s
        return act, s + act * (1.0 - s)

    for p in range(2):
        rows = pl.ds(p * ROWS, ROWS)
        if p == 1:
            got_feat.wait_recv()

        @pl.loop(0, H // C1)
        def _(n):
            cols = chunk(n, C1)
            val = tn(feat[rows, :], win[:, cols]) + stats[0:1, cols]
            act, slope = silu_both(val)
            act1[rows, cols] = act.astype(BF)
            sl1[rows, cols] = slope.astype(BF)

        accq[rows, :] = jnp.zeros((ROWS, 128), F32)
        if p == 0:
            for copy in loads[2:]:
                copy.wait()

        @pl.loop(0, H // C2)
        def _(n):
            cols = chunk(n, C2)
            val = tn(act1[rows, :], wmid[:, cols]) + stats[1:2, cols]
            act, slope = silu_both(val)
            wrow = stats[2:3, cols]
            prod = act * wrow
            accq[rows, :] += sum(prod[:, i * 128 : (i + 1) * 128] for i in range(C2 // 128))
            act2[rows, cols] = act.astype(BF)
            sl2[rows, cols] = (slope * wrow).astype(BF)

    q = nt(jnp.ones((8, 128), F32), accq[...], precision=lax.Precision.HIGHEST)
    got_tgt.wait_recv()
    qm[...] = q[:, ROWS:]
    mo[...] = q[:, :ROWS]
    got_q = send(qm, qr, v3)
    err = q - jnp.concatenate([tgt[...], tgtm[...]], axis=1)
    eb[...] = jnp.transpose(jnp.broadcast_to(err[0:1], (128, R2)))
    stats[...] = jnp.zeros_like(stats)

    @pl.loop(0, H // C3)
    def _(n):
        cols = chunk(n, C3)
        e = jnp.concatenate([eb[...]] * (C3 // 128), axis=1)
        d = e * sl2[:, cols].astype(F32)
        del2[:, cols] = d.astype(BF)
        stats[1:2, cols] = jnp.sum(d, axis=0, keepdims=True)
        stats[2:3, cols] = jnp.sum(e * act2[:, cols].astype(F32), axis=0, keepdims=True)

    order = (2, 1, 3, 0)

    def group(ru):
        for rv in range(4):
            lhs[pl.ds(rv * 128, 128), :] = jnp.transpose(act1[:, chunk(dp_of(ru, rv), 128)])

    def products(ru, half):
        cols = pl.ds(half * HALF, HALF)
        res = tn(lhs[...], del2[:, cols]).astype(BF)
        for rv in range(4):
            part[ru, rv, :, cols] = res[rv * 128 : (rv + 1) * 128]

    left, right = pl.ds(0, HALF), pl.ds(HALF, HALF)
    one_a, one_b, two_a, two_b = [None] * 4, [None] * 4, [None] * 4, [None] * 4
    group(2)
    products(2, 0)
    for rv in order:
        one_a[rv] = send(part.at[2, rv, :, left], r1a.at[rv], u1)
    products(2, 1)
    for rv in order:
        one_b[rv] = send(part.at[2, rv, :, right], r1b.at[rv], u3)
    group(1)
    products(1, 0)
    for rv in order:
        two_a[rv] = [send(part.at[1, rv, :, left], r2a.at[rv, :, left], u1)]
    products(1, 1)
    group(3)
    products(3, 1)
    for rv in order:
        two_b[rv] = [send(part.at[3, rv, :, right], r2b.at[rv, :, right], u3)]
    products(3, 0)
    group(0)
    products(0, 0)
    products(0, 1)

    got_q.wait_recv()
    mo[...] = jnp.minimum(mo[...], qr[...])
    got_sib = send(mo, ms, sib)

    def merge():
        for rv in order:
            one_a[rv].wait_recv()
            part[3, rv, :, left] = (part[3, rv, :, left].astype(F32) + r1a[rv].astype(F32)).astype(BF)
            two_b[rv].append(send(part.at[3, rv, :, left], r2b.at[rv, :, left], u3))
            one_b[rv].wait_recv()
            part[1, rv, :, right] = (part[1, rv, :, right].astype(F32) + r1b[rv].astype(F32)).astype(BF)
            two_a[rv].append(send(part.at[1, rv, :, right], r2a.at[rv, :, right], u1))

    featT[...] = jnp.transpose(feat[...])

    @pl.loop(0, H // C5)
    def _(n):
        cols = chunk(n, C5)
        back = nt(del2[...], wmid[cols, :])
        d = back * sl1[:, cols].astype(F32)
        stats[0:1, cols] = jnp.sum(d, axis=0, keepdims=True)
        res = tn(featT[...], d.astype(BF)).astype(BF)
        for i in range(16):
            slot = jnp.where(core == 0, (i // 4 ^ y) * 4 + (i % 4 ^ z), (i % 4 ^ z) * 4 + (i // 4 ^ y))
            gp[slot, :, cols] = res[i * 16 : (i + 1) * 16]

    for i in range(16):
        slot = jnp.where(core == 0, (i // 4 ^ y) * 4 + (i % 4 ^ z), (i % 4 ^ z) * 4 + (i // 4 ^ y))
        tile = jnp.concatenate([stats[:, i * 128 : (i + 1) * 128], jnp.zeros((8, 128), F32)], axis=0)
        gp[slot, :, pl.ds(H, 128)] = tile.astype(BF)
        gp[slot, :, pl.ds(H + 128, 128)] = jnp.zeros((16, 128), BF)

    got_sib.wait_recv()
    mm[...] = jnp.minimum(mo[...], ms[...])
    got_x = [send(mm, mx.at[k], xs[k]) for k in range(3)]

    gl, gr = pl.ds(0, GH), pl.ds(GH, GH)
    g_one_a = send(gp.at[pl.ds(8, 4), :, gl], g1a, u1)
    g_one_b = send(gp.at[pl.ds(8, 4), :, gr], g1b, u3)
    g_two_a = [send(gp.at[pl.ds(4, 4), :, gl], g2a.at[:, :, gl], u1)]
    g_two_b = [send(gp.at[pl.ds(12, 4), :, gr], g2b.at[:, :, gr], u3)]

    merge()

    g_one_a.wait_recv()
    gp[12:16, :, gl] = (gp[12:16, :, gl].astype(F32) + g1a[...].astype(F32)).astype(BF)
    g_two_b.append(send(gp.at[pl.ds(12, 4), :, gl], g2b.at[:, :, gl], u3))
    g_one_b.wait_recv()
    gp[4:8, :, gr] = (gp[4:8, :, gr].astype(F32) + g1b[...].astype(F32)).astype(BF)
    g_two_a.append(send(gp.at[pl.ds(4, 4), :, gr], g2a.at[:, :, gr], u1))

    sides = (left, right)

    def ring_sum(rv, half):
        two_a[rv][half].wait_recv()
        two_b[rv][1 - half].wait_recv()
        at = sides[half]
        return part[0, rv, :, at].astype(F32) + r2a[rv, :, at].astype(F32) + r2b[rv, :, at].astype(F32)

    three = {}
    for rv, slot in ((2, 1), (1, 0)):
        for half, at in enumerate(sides):
            part[0, rv, :, at] = ring_sum(rv, half).astype(BF)
            three[slot, half] = send(part.at[0, rv, :, at], r3.at[slot, :, at], v1)
    four = []
    for half, at in enumerate(sides):
        total = ring_sum(3, half)
        three[1, half].wait_recv()
        part[0, 3, :, at] = (total + r3[1, :, at].astype(F32)).astype(BF)
        four.append(send(part.at[0, 3, :, at], mid_out.at[head, :, at], v3))

    for copy in (*g_two_a, *g_two_b):
        copy.wait_recv()
    gp[0:4] = (gp[0:4].astype(F32) + g2a[...].astype(F32) + g2b[...].astype(F32)).astype(BF)
    g_three = send(gp.at[pl.ds(1, 2)], g3, v1)

    own_mid = []
    for half, at in enumerate(sides):
        total = ring_sum(0, half)
        three[0, half].wait_recv()
        part[0, 0, :, at] = (total + r3[0, :, at].astype(F32)).astype(BF)
        copy = pltpu.make_async_copy(part.at[0, 0, :, at], mid_out.at[head, :, at], osem.at[half])
        copy.start()
        own_mid.append(copy)

    g_three.wait_recv()
    gp[3] = (gp[3].astype(F32) + g3[1].astype(F32)).astype(BF)
    g_four = send(gp.at[3], gin_out.at[head], v3)
    gp[0] = (gp[0].astype(F32) + g3[0].astype(F32)).astype(BF)
    own_gin = pltpu.make_async_copy(gp.at[0], gin_out.at[head], osem.at[2])
    own_gin.start()

    for copy in got_x:
        copy.wait_recv()
    q_min = jnp.minimum(jnp.minimum(mm[...], mx[0]), jnp.minimum(mx[1], mx[2]))
    gap = q_min[0:1] - vnow[...].reshape(1, ROWS)
    vg_out[...] = -2.0 * jnp.where(gap < 0.0, 0.3, 0.7) * gap

    for copy in own_mid:
        copy.wait()
    own_gin.wait()
    for copy in four:
        copy.wait_recv()
    g_four.wait_recv()
    for copy in copies:
        copy.wait_send()


def finish(vg, mid, gin, vg_out, din, dmid, dbias, dout):
    vg_out[...] = vg[...].reshape(ROWS)
    for h in range(2):
        dmid[:, h, :] = mid[h].astype(F32)
        din[:, h, :] = gin[h, :, :H].astype(F32)
        rest = gin[h, :, H : H + 128].astype(F32)
        dbias[0, h : h + 1, :] = rest[0:1]
        dbias[1, h : h + 1, :] = rest[1:2]
        dout[h : h + 1, :] = rest[2:3]


def per_device(features, reward, done, value_next, value_now, w_in, w_mid, biases, w_out):
    vm = pl.BlockSpec(memory_space=pltpu.VMEM)
    hbm = pl.BlockSpec(memory_space=pl.ANY)
    line = (1, ROWS)
    vg, mid, gin = pl.pallas_call(
        kernel,
        out_shape=(
            jax.ShapeDtypeStruct(line, F32),
            jax.ShapeDtypeStruct((2, 128, H), BF),
            jax.ShapeDtypeStruct((2, 16, GW), BF),
        ),
        in_specs=[hbm, vm, vm, vm, vm, hbm, hbm, vm, vm],
        out_specs=(vm, hbm, hbm),
        scratch_shapes=[
            pltpu.VMEM((R2, IN), BF),
            pltpu.VMEM((IN, H), BF),
            pltpu.VMEM((H, H), BF),
            pltpu.VMEM((R2, H), BF),
            pltpu.VMEM((R2, H), BF),
            pltpu.VMEM((R2, H), BF),
            pltpu.VMEM((R2, H), BF),
            pltpu.VMEM((R2, H), BF),
            pltpu.VMEM((R2, 128), F32),
            pltpu.VMEM((R2, 128), F32),
            pltpu.VMEM((8, H), F32),
            pltpu.VMEM((4, 4, 128, H), BF),
            pltpu.VMEM((512, R2), BF),
            pltpu.VMEM((IN, R2), BF),
            pltpu.VMEM((4, 128, HALF), BF),
            pltpu.VMEM((4, 128, HALF), BF),
            pltpu.VMEM((4, 128, H), BF),
            pltpu.VMEM((4, 128, H), BF),
            pltpu.VMEM((2, 128, H), BF),
            pltpu.VMEM((16, 16, GW), BF),
            pltpu.VMEM((4, 16, GH), BF),
            pltpu.VMEM((4, 16, GH), BF),
            pltpu.VMEM((4, 16, GW), BF),
            pltpu.VMEM((4, 16, GW), BF),
            pltpu.VMEM((2, 16, GW), BF),
            *[pltpu.VMEM((8, ROWS), F32)] * 7,
            pltpu.VMEM((3, 8, ROWS), F32),
            pltpu.SemaphoreType.DMA((2,)),
            pltpu.SemaphoreType.DMA((NC,)),
            pltpu.SemaphoreType.DMA((3,)),
            pltpu.SemaphoreType.DMA((56,)),
            pltpu.SemaphoreType.DMA((56,)),
        ],
        compiler_params=pltpu.CompilerParams(
            collective_id=0, has_side_effects=True, vmem_limit_bytes=67_000_000
        ),
    )(
        features, reward, done, value_next, value_now, w_in, w_mid, biases, w_out,
    )
    return pl.pallas_call(
        finish,
        out_shape=(
            jax.ShapeDtypeStruct((ROWS,), F32),
            jax.ShapeDtypeStruct((16, 2, H), F32),
            jax.ShapeDtypeStruct((128, 2, H), F32),
            jax.ShapeDtypeStruct((2, 2, 128), F32),
            jax.ShapeDtypeStruct((2, 128), F32),
        ),
        in_specs=[vm, vm, vm],
        out_specs=(vm,) * 5,
    )(vg, mid, gin)


def solution(mesh):
    in_specs = (
        P("dp", None), P("dp"), P("dp"), P("dp"), P("dp"),
        P("ens", None, None), P("ens", None, None), P(None, "ens", None), P("ens", None),
    )
    out_specs = (
        P("dp"), P("dp", "ens", None), P("dp", "ens", None), P(None, "ens", "dp"), P("ens", "dp"),
    )
    return jax.shard_map(
        per_device, mesh=mesh, in_specs=in_specs, out_specs=out_specs, check_vma=False
    )
```

```python
import jax
import jax.numpy as jnp
from jax import lax
from jax.experimental import pallas as pl
from jax.experimental.pallas import tpu as pltpu
from jax.sharding import PartitionSpec as P

MESH = pl.DeviceIdType.MESH
BF = jnp.bfloat16
F32 = jnp.float32
ROWS = 384
IN = 256
H = 2048
R2 = 2 * ROWS
C = 256
NC = H // C
C1 = 512
C2 = 512
C3 = 512
C5 = 512
GW = H + 128
LEFT = 768
RIGHT = H - LEFT
GL = 896
GR = GW - GL


def tn(a, b, **kw):
    return lax.dot_general(a, b, (((1,), (0,)), ((), ())), preferred_element_type=F32, **kw)


def nt(a, b, **kw):
    return lax.dot_general(a, b, (((1,), (1,)), ((), ())), preferred_element_type=F32, **kw)


def chunk(n, width=C):
    return pl.ds(pl.multiple_of(n * width, width), width)


def kernel(
    feat_hbm, reward_hbm, done_hbm, vnext_hbm, vnow_hbm, win_hbm, wmid_hbm, biases_hbm, wout_hbm,
    vg_out, mid_out, gin_out,
    feat, win, wmid, act1, sl1, act2, sl2, del2, accq, eb, stats, part, actT, featT,
    r1a, r1b, r2a, r2b, r3, gp, g1a, g1b, g2a, g2b, g3,
    reward, done, vnext, vnow, biases, wout, tgt, tgtm, qm, qr, mo, ms, mm, mx,
    lsem, wsem, osem, ssem, rsem,
):
    ens = lax.axis_index("ens")
    dp = lax.axis_index("dp")
    core = lax.rem(ens, 2)
    xpos = lax.div(ens, 2)
    y = lax.div(dp, 4)
    z = lax.rem(dp, 4)
    u = jnp.where(core == 0, y, z)
    v = jnp.where(core == 0, z, y)
    su = 4 - 3 * core
    sv = 1 + 3 * core
    head = lax.div(v, 2)

    def dp_of(ru, rv):
        return (u ^ ru) * su + (v ^ rv) * sv

    def dev(ru, rv):
        return (ens, dp_of(ru, rv))

    u1, u3, v1, v3 = dev(1, 0), dev(3, 0), dev(0, 1), dev(0, 3)
    sib = (ens ^ 1, dp)
    xs = [((xpos ^ k) * 2 + core, dp) for k in (1, 2, 3)]

    barrier = pltpu.get_barrier_semaphore()
    partners = [u1, u3, v1, v3, sib, *xs]
    for p in partners:
        pl.semaphore_signal(barrier, inc=1, device_id=p, device_id_type=MESH)

    loads = [
        pltpu.make_async_copy(feat_hbm, feat.at[pl.ds(0, ROWS)], lsem.at[0]),
        pltpu.make_async_copy(win_hbm.at[head], win, lsem.at[1]),
    ]
    for n in range(NC):
        loads.append(
            pltpu.make_async_copy(
                wmid_hbm.at[head, :, pl.ds(n * C, C)], wmid.at[:, pl.ds(n * C, C)], wsem.at[n]
            )
        )
    for copy in loads[:2]:
        copy.start()

    small = [
        pltpu.make_async_copy(src, dst, lsem.at[2 + i])
        for i, (src, dst) in enumerate(
            (
                (biases_hbm, biases), (wout_hbm, wout), (reward_hbm, reward), (done_hbm, done),
                (vnext_hbm, vnext), (vnow_hbm, vnow),
            )
        )
    ]
    for copy in small:
        copy.start()

    for copy in loads[2:]:
        copy.start()

    for copy in small:
        copy.wait()
    target = reward[...] + 0.99 * (1.0 - done[...].astype(F32)) * vnext[...]
    tgt[...] = jnp.broadcast_to(target.reshape(1, ROWS), (8, ROWS))
    loads[0].wait()
    loads[1].wait()

    wo = wout[...].astype(F32)
    wo = jnp.where(head == 0, wo[0:1], wo[1:2])
    b_all = biases[...]
    b_one = jnp.where(head == 0, b_all[0, 0:1], b_all[0, 1:2])
    b_two = jnp.where(head == 0, b_all[1, 0:1], b_all[1, 1:2])
    stats[...] = jnp.zeros_like(stats)
    stats[0:1, :] = b_one
    stats[1:2, :] = b_two
    stats[2:3, :] = wo

    def silu_both(val):
        s = 0.5 * jnp.tanh(0.5 * val) + 0.5
        act = val * s
        return act, s + act * (1.0 - s)

    accq[...] = jnp.zeros_like(accq)

    def layer_one(p):
        rows = pl.ds(p * ROWS, ROWS)

        @pl.loop(0, H // C1)
        def _(n):
            cols = chunk(n, C1)
            val = tn(feat[rows, :], win[:, cols]) + stats[0:1, cols]
            act, slope = silu_both(val)
            act1[rows, cols] = act.astype(BF)
            sl1[rows, cols] = slope.astype(BF)

    pl.semaphore_wait(barrier, len(partners))

    copies = []

    def send(src, dst, to):
        i = len(copies)
        copy = pltpu.make_async_remote_copy(
            src_ref=src, dst_ref=dst, send_sem=ssem.at[i], recv_sem=rsem.at[i],
            device_id=to, device_id_type=MESH,
        )
        copies.append(copy)
        copy.start()
        return copy

    got_feat = send(feat.at[pl.ds(0, ROWS)], feat.at[pl.ds(ROWS, ROWS)], v3)
    got_tgt = send(tgt, tgtm, v3)
    def layer_two(p):
        rows = pl.ds(p * ROWS, ROWS)

        @pl.loop(0, H // C2)
        def _(n):
            cols = chunk(n, C2)
            if p == 1:
                for i in range(C2 // 128):
                    d = n * (C2 // 128) + i
                    actT[d] = jnp.transpose(act1[:, chunk(d, 128)])
            val = tn(act1[rows, :], wmid[:, cols]) + stats[1:2, cols]
            act, slope = silu_both(val)
            wrow = stats[2:3, cols]
            prod = act * wrow
            accq[rows, :] += sum(prod[:, i * 128 : (i + 1) * 128] for i in range(C2 // 128))
            act2[rows, cols] = act.astype(BF)
            sl2[rows, cols] = (slope * wrow).astype(BF)

    layer_one(0)
    for copy in loads[2:]:
        copy.wait()
    layer_two(0)
    got_feat.wait_recv()
    layer_one(1)
    layer_two(1)

    q = nt(jnp.ones((8, 128), F32), accq[...], precision=lax.Precision.HIGHEST)
    got_tgt.wait_recv()
    qm[...] = q[:, ROWS:]
    mo[...] = q[:, :ROWS]
    got_q = send(qm, qr, v3)
    err = q - jnp.concatenate([tgt[...], tgtm[...]], axis=1)
    eb[...] = jnp.transpose(jnp.broadcast_to(err[0:1], (128, R2)))
    stats[...] = jnp.zeros_like(stats)

    @pl.loop(0, H // C3)
    def _(n):
        cols = chunk(n, C3)
        e = jnp.concatenate([eb[...]] * (C3 // 128), axis=1)
        d = e * sl2[:, cols].astype(F32)
        del2[:, cols] = d.astype(BF)
        stats[1:2, cols] = jnp.sum(d, axis=0, keepdims=True)
        stats[2:3, cols] = jnp.sum(e * act2[:, cols].astype(F32), axis=0, keepdims=True)

    order = (2, 1, 3, 0)

    def products(ru, side):
        rows = jnp.concatenate([actT[dp_of(ru, rv)] for rv in range(4)], axis=0)
        res = tn(rows, del2[:, side]).astype(BF)
        for rv in range(4):
            part[ru, rv, :, side] = res[rv * 128 : (rv + 1) * 128]

    left, right = pl.ds(0, LEFT), pl.ds(LEFT, RIGHT)
    one_a, one_b, two_a, two_b = [None] * 4, [None] * 4, [None] * 4, [None] * 4
    first, last = (2, 1), (3, 0)

    def step_one(side, rvs):
        for rv in rvs:
            if side == 0:
                one_a[rv] = send(part.at[2, rv, :, left], r1a.at[rv], u1)
            else:
                one_b[rv] = send(part.at[2, rv, :, right], r1b.at[rv], u3)

    def raw(side, rvs):
        for rv in rvs:
            if side == 0:
                two_a[rv] = [send(part.at[1, rv, :, left], r2a.at[rv, :, left], u1)]
            else:
                two_b[rv] = [send(part.at[3, rv, :, right], r2b.at[rv, :, right], u3)]

    def merge(rvs):
        for rv in rvs:
            one_a[rv].wait_recv()
            part[3, rv, :, left] = (part[3, rv, :, left].astype(F32) + r1a[rv].astype(F32)).astype(BF)
            two_b[rv].append(send(part.at[3, rv, :, left], r2b.at[rv, :, left], u3))
            one_b[rv].wait_recv()
            part[1, rv, :, right] = (part[1, rv, :, right].astype(F32) + r1b[rv].astype(F32)).astype(BF)
            two_a[rv].append(send(part.at[1, rv, :, right], r2a.at[rv, :, right], u1))

    products(2, right)
    step_one(1, order)
    products(2, left)
    step_one(0, order)
    products(1, left)
    raw(0, first)

    featT[...] = jnp.transpose(feat[...])

    @pl.loop(0, H // C5)
    def _(n):
        cols = chunk(n, C5)
        back = nt(del2[...], wmid[cols, :])
        d = back * sl1[:, cols].astype(F32)
        stats[0:1, cols] = jnp.sum(d, axis=0, keepdims=True)
        res = tn(featT[...], d.astype(BF)).astype(BF)
        for i in range(16):
            slot = jnp.where(core == 0, (i // 4 ^ y) * 4 + (i % 4 ^ z), (i % 4 ^ z) * 4 + (i // 4 ^ y))
            gp[slot, :, cols] = res[i * 16 : (i + 1) * 16]

    for i in range(16):
        slot = jnp.where(core == 0, (i // 4 ^ y) * 4 + (i % 4 ^ z), (i % 4 ^ z) * 4 + (i // 4 ^ y))
        tile = jnp.concatenate([stats[:, i * 128 : (i + 1) * 128], jnp.zeros((8, 128), F32)], axis=0)
        gp[slot, :, pl.ds(H, 128)] = tile.astype(BF)

    gl, gr = pl.ds(0, GL), pl.ds(GL, GR)
    g_one_a = send(gp.at[pl.ds(8, 4), :, gl], g1a, u1)
    g_one_b = send(gp.at[pl.ds(8, 4), :, gr], g1b, u3)
    g_two_a = [send(gp.at[pl.ds(4, 4), :, gl], g2a.at[:, :, gl], u1)]
    g_two_b = [send(gp.at[pl.ds(12, 4), :, gr], g2b.at[:, :, gr], u3)]

    got_q.wait_recv()
    mo[...] = jnp.minimum(mo[...], qr[...])
    got_sib = send(mo, ms, sib)

    products(3, right)
    raw(1, first)
    products(1, right)
    products(3, left)
    g_one_a.wait_recv()
    gp[12:16, :, gl] = (gp[12:16, :, gl].astype(F32) + g1a[...].astype(F32)).astype(BF)
    g_two_b.append(send(gp.at[pl.ds(12, 4), :, gl], g2b.at[:, :, gl], u3))
    g_one_b.wait_recv()
    gp[4:8, :, gr] = (gp[4:8, :, gr].astype(F32) + g1b[...].astype(F32)).astype(BF)
    g_two_a.append(send(gp.at[pl.ds(4, 4), :, gr], g2a.at[:, :, gr], u1))
    merge(first)
    raw(0, last)
    raw(1, last)
    merge(last)
    got_sib.wait_recv()
    mm[...] = jnp.minimum(mo[...], ms[...])
    got_x = [send(mm, mx.at[k], xs[k]) for k in range(3)]
    products(0, left)
    products(0, right)

    sides = (left, right)

    def ring_sum(rv, half):
        two_a[rv][half].wait_recv()
        two_b[rv][1 - half].wait_recv()
        at = sides[half]
        return part[0, rv, :, at].astype(F32) + r2a[rv, :, at].astype(F32) + r2b[rv, :, at].astype(F32)

    three = {}
    for rv, slot in ((2, 1), (1, 0)):
        for half, at in enumerate(sides):
            part[0, rv, :, at] = ring_sum(rv, half).astype(BF)
            three[slot, half] = send(part.at[0, rv, :, at], r3.at[slot, :, at], v1)
    for copy in (*g_two_a, *g_two_b):
        copy.wait_recv()
    gp[0:4] = (gp[0:4].astype(F32) + g2a[...].astype(F32) + g2b[...].astype(F32)).astype(BF)
    g_three = send(gp.at[pl.ds(1, 2)], g3, v1)

    four = []
    for half, at in enumerate(sides):
        total = ring_sum(3, half)
        three[1, half].wait_recv()
        part[0, 3, :, at] = (total + r3[1, :, at].astype(F32)).astype(BF)
        four.append(send(part.at[0, 3, :, at], mid_out.at[head, :, at], v3))

    g_three.wait_recv()
    gp[3] = (gp[3].astype(F32) + g3[1].astype(F32)).astype(BF)
    g_four = send(gp.at[3], gin_out.at[head], v3)
    gp[0] = (gp[0].astype(F32) + g3[0].astype(F32)).astype(BF)
    own_gin = pltpu.make_async_copy(gp.at[0], gin_out.at[head], osem.at[2])
    own_gin.start()

    own_mid = []
    for half, at in enumerate(sides):
        total = ring_sum(0, half)
        three[0, half].wait_recv()
        part[0, 0, :, at] = (total + r3[0, :, at].astype(F32)).astype(BF)
        copy = pltpu.make_async_copy(part.at[0, 0, :, at], mid_out.at[head, :, at], osem.at[half])
        copy.start()
        own_mid.append(copy)

    for copy in got_x:
        copy.wait_recv()
    q_min = jnp.minimum(jnp.minimum(mm[...], mx[0]), jnp.minimum(mx[1], mx[2]))
    gap = q_min[0:1] - vnow[...].reshape(1, ROWS)
    vg_out[...] = -2.0 * jnp.where(gap < 0.0, 0.3, 0.7) * gap

    for copy in own_mid:
        copy.wait()
    own_gin.wait()
    for copy in four:
        copy.wait_recv()
    g_four.wait_recv()
    for copy in copies:
        copy.wait_send()


def finish(vg, mid, gin, vg_out, din, dmid, dbias, dout):
    for h in range(2):
        dmid[:, h, :] = mid[h].astype(F32)

    @pl.when(pl.program_id(0) == 0)
    def _():
        vg_out[...] = vg[...].reshape(ROWS)
        for h in range(2):
            din[:, h, :] = gin[h, :, :H].astype(F32)
            rest = gin[h, :, H:].astype(F32)
            dbias[0, h : h + 1, :] = rest[0:1]
            dbias[1, h : h + 1, :] = rest[1:2]
            dout[h : h + 1, :] = rest[2:3]


def per_device(features, reward, done, value_next, value_now, w_in, w_mid, biases, w_out):
    vm = pl.BlockSpec(memory_space=pltpu.VMEM)
    hbm = pl.BlockSpec(memory_space=pl.ANY)
    line = (1, ROWS)
    vg, mid, gin = pl.pallas_call(
        kernel,
        out_shape=(
            jax.ShapeDtypeStruct(line, F32),
            jax.ShapeDtypeStruct((2, 128, H), BF),
            jax.ShapeDtypeStruct((2, 16, GW), BF),
        ),
        in_specs=[hbm] * 9,
        out_specs=(vm, hbm, hbm),
        scratch_shapes=[
            pltpu.VMEM((R2, IN), BF),
            pltpu.VMEM((IN, H), BF),
            pltpu.VMEM((H, H), BF),
            pltpu.VMEM((R2, H), BF),
            pltpu.VMEM((R2, H), BF),
            pltpu.VMEM((R2, H), BF),
            pltpu.VMEM((R2, H), BF),
            pltpu.VMEM((R2, H), BF),
            pltpu.VMEM((R2, 128), F32),
            pltpu.VMEM((R2, 128), F32),
            pltpu.VMEM((8, H), F32),
            pltpu.VMEM((4, 4, 128, H), BF),
            pltpu.VMEM((16, 128, R2), BF),
            pltpu.VMEM((IN, R2), BF),
            pltpu.VMEM((4, 128, LEFT), BF),
            pltpu.VMEM((4, 128, RIGHT), BF),
            pltpu.VMEM((4, 128, H), BF),
            pltpu.VMEM((4, 128, H), BF),
            pltpu.VMEM((2, 128, H), BF),
            pltpu.VMEM((16, 16, GW), BF),
            pltpu.VMEM((4, 16, GL), BF),
            pltpu.VMEM((4, 16, GR), BF),
            pltpu.VMEM((4, 16, GW), BF),
            pltpu.VMEM((4, 16, GW), BF),
            pltpu.VMEM((2, 16, GW), BF),
            pltpu.VMEM((ROWS,), F32),
            pltpu.VMEM((ROWS,), jnp.int32),
            pltpu.VMEM((ROWS,), F32),
            pltpu.VMEM((ROWS,), F32),
            pltpu.VMEM((2, 2, H), F32),
            pltpu.VMEM((2, H), BF),
            *[pltpu.VMEM((8, ROWS), F32)] * 7,
            pltpu.VMEM((3, 8, ROWS), F32),
            pltpu.SemaphoreType.DMA((8,)),
            pltpu.SemaphoreType.DMA((NC,)),
            pltpu.SemaphoreType.DMA((3,)),
            pltpu.SemaphoreType.DMA((56,)),
            pltpu.SemaphoreType.DMA((56,)),
        ],
        compiler_params=pltpu.CompilerParams(
            collective_id=0, has_side_effects=True, vmem_limit_bytes=67_000_000
        ),
    )(
        features, reward, done, value_next, value_now, w_in, w_mid, biases, w_out,
    )
    return pl.pallas_call(
        finish,
        out_shape=(
            jax.ShapeDtypeStruct((ROWS,), F32),
            jax.ShapeDtypeStruct((16, 2, H), F32),
            jax.ShapeDtypeStruct((128, 2, H), F32),
            jax.ShapeDtypeStruct((2, 2, 128), F32),
            jax.ShapeDtypeStruct((2, 128), F32),
        ),
        grid=(4,),
        in_specs=[vm, pl.BlockSpec((2, 32, H), lambda i: (0, i, 0)), vm],
        out_specs=(vm, vm, pl.BlockSpec((32, 2, H), lambda i: (i, 0, 0)), vm, vm),
    )(vg, mid, gin)


def solution(mesh):
    in_specs = (
        P("dp", None), P("dp"), P("dp"), P("dp"), P("dp"),
        P("ens", None, None), P("ens", None, None), P(None, "ens", None), P("ens", None),
    )
    out_specs = (
        P("dp"), P("dp", "ens", None), P("dp", "ens", None), P(None, "ens", "dp"), P("ens", "dp"),
    )
    return jax.shard_map(
        per_device, mesh=mesh, in_specs=in_specs, out_specs=out_specs, check_vma=False
    )
```

```python
import jax
import jax.numpy as jnp
from jax import lax
from jax.experimental import pallas as pl
from jax.experimental.pallas import tpu as pltpu
from jax.sharding import PartitionSpec as P

MESH = pl.DeviceIdType.MESH
BF = jnp.bfloat16
F32 = jnp.float32
ROWS = 384
IN = 256
H = 2048
R2 = 2 * ROWS
C = 256
NC = H // C
C1 = 512
C2 = 512
C3 = 512
C5 = 512
GW = H + 128
LEFT = 768
RIGHT = H - LEFT
GL = 896
GR = GW - GL


def tn(a, b, **kw):
    return lax.dot_general(a, b, (((1,), (0,)), ((), ())), preferred_element_type=F32, **kw)


def nt(a, b, **kw):
    return lax.dot_general(a, b, (((1,), (1,)), ((), ())), preferred_element_type=F32, **kw)


def chunk(n, width=C):
    return pl.ds(pl.multiple_of(n * width, width), width)


def kernel(
    feat_hbm, reward_hbm, done_hbm, vnext_hbm, vnow_hbm, win_hbm, wmid_hbm, biases_hbm, wout_hbm,
    vg_out, mid_out, gin_out,
    feat, win, wmid, act1, sl1, act2, sl2, del2, accq, eb, stats, part, actT, featT,
    r1a, r1b, r2a, r2b, r3, gp, g1a, g1b, g2a, g2b, g3,
    reward, done, vnext, vnow, biases, wout, tgt, tgtm, qm, qr, mo, ms, mm, mx,
    lsem, wsem, osem, ssem, rsem,
):
    ens = lax.axis_index("ens")
    dp = lax.axis_index("dp")
    core = lax.rem(ens, 2)
    xpos = lax.div(ens, 2)
    y = lax.div(dp, 4)
    z = lax.rem(dp, 4)
    u = jnp.where(core == 0, y, z)
    v = jnp.where(core == 0, z, y)
    su = 4 - 3 * core
    sv = 1 + 3 * core
    head = lax.div(v, 2)

    def dp_of(ru, rv):
        return (u ^ ru) * su + (v ^ rv) * sv

    def dev(ru, rv):
        return (ens, dp_of(ru, rv))

    u1, u3, v1, v3 = dev(1, 0), dev(3, 0), dev(0, 1), dev(0, 3)
    sib = (ens ^ 1, dp)
    xs = [((xpos ^ k) * 2 + core, dp) for k in (1, 2, 3)]

    barrier = pltpu.get_barrier_semaphore()
    partners = [u1, u3, v1, v3, sib, *xs]
    for p in partners:
        pl.semaphore_signal(barrier, inc=1, device_id=p, device_id_type=MESH)

    loads = [
        pltpu.make_async_copy(feat_hbm, feat.at[pl.ds(0, ROWS)], lsem.at[0]),
        pltpu.make_async_copy(win_hbm.at[head], win, lsem.at[1]),
    ]
    for n in range(NC):
        loads.append(
            pltpu.make_async_copy(
                wmid_hbm.at[head, :, pl.ds(n * C, C)], wmid.at[:, pl.ds(n * C, C)], wsem.at[n]
            )
        )
    for copy in loads[:2]:
        copy.start()

    small = [
        pltpu.make_async_copy(src, dst, lsem.at[2 + i])
        for i, (src, dst) in enumerate(
            (
                (biases_hbm, biases), (wout_hbm, wout), (reward_hbm, reward), (done_hbm, done),
                (vnext_hbm, vnext), (vnow_hbm, vnow),
            )
        )
    ]
    for copy in small:
        copy.start()

    for copy in loads[2:]:
        copy.start()

    for copy in small:
        copy.wait()
    target = reward[...] + 0.99 * (1.0 - done[...].astype(F32)) * vnext[...]
    tgt[...] = jnp.broadcast_to(target.reshape(1, ROWS), (8, ROWS))
    loads[0].wait()
    loads[1].wait()

    wo = wout[...].astype(F32)
    wo = jnp.where(head == 0, wo[0:1], wo[1:2])
    b_all = biases[...]
    b_one = jnp.where(head == 0, b_all[0, 0:1], b_all[0, 1:2])
    b_two = jnp.where(head == 0, b_all[1, 0:1], b_all[1, 1:2])
    stats[...] = jnp.zeros_like(stats)
    stats[0:1, :] = b_one
    stats[1:2, :] = b_two
    stats[2:3, :] = wo

    def silu_both(val):
        s = 0.5 * jnp.tanh(0.5 * val) + 0.5
        act = val * s
        return act, s + act * (1.0 - s)

    accq[...] = jnp.zeros_like(accq)

    def layer_one(p):
        rows = pl.ds(p * ROWS, ROWS)

        @pl.loop(0, H // C1)
        def _(n):
            cols = chunk(n, C1)
            val = tn(feat[rows, :], win[:, cols]) + stats[0:1, cols]
            act, slope = silu_both(val)
            act1[rows, cols] = act.astype(BF)
            sl1[rows, cols] = slope.astype(BF)

    pl.semaphore_wait(barrier, len(partners))

    copies = []

    def send(src, dst, to):
        i = len(copies)
        copy = pltpu.make_async_remote_copy(
            src_ref=src, dst_ref=dst, send_sem=ssem.at[i], recv_sem=rsem.at[i],
            device_id=to, device_id_type=MESH,
        )
        copies.append(copy)
        copy.start()
        return copy

    got_feat = send(feat.at[pl.ds(0, ROWS)], feat.at[pl.ds(ROWS, ROWS)], v3)
    got_tgt = send(tgt, tgtm, v3)
    def layer_two(p):
        rows = pl.ds(p * ROWS, ROWS)

        @pl.loop(0, H // C2)
        def _(n):
            cols = chunk(n, C2)
            if p == 1:
                for i in range(C2 // 128):
                    d = n * (C2 // 128) + i
                    actT[d] = jnp.transpose(act1[:, chunk(d, 128)])
            val = tn(act1[rows, :], wmid[:, cols]) + stats[1:2, cols]
            act, slope = silu_both(val)
            wrow = stats[2:3, cols]
            prod = act * wrow
            accq[rows, :] += sum(prod[:, i * 128 : (i + 1) * 128] for i in range(C2 // 128))
            act2[rows, cols] = act.astype(BF)
            sl2[rows, cols] = (slope * wrow).astype(BF)

    layer_one(0)
    for copy in loads[2:]:
        copy.wait()
    layer_two(0)
    got_feat.wait_recv()
    layer_one(1)
    layer_two(1)

    q = nt(jnp.ones((8, 128), F32), accq[...], precision=lax.Precision.HIGHEST)
    got_tgt.wait_recv()
    qm[...] = q[:, ROWS:]
    mo[...] = q[:, :ROWS]
    got_q = send(qm, qr, v3)
    err = q - jnp.concatenate([tgt[...], tgtm[...]], axis=1)
    eb[...] = jnp.transpose(jnp.broadcast_to(err[0:1], (128, R2)))
    stats[...] = jnp.zeros_like(stats)

    @pl.loop(0, H // C3)
    def _(n):
        cols = chunk(n, C3)
        e = jnp.concatenate([eb[...]] * (C3 // 128), axis=1)
        d = e * sl2[:, cols].astype(F32)
        del2[:, cols] = d.astype(BF)
        stats[1:2, cols] = jnp.sum(d, axis=0, keepdims=True)
        stats[2:3, cols] = jnp.sum(e * act2[:, cols].astype(F32), axis=0, keepdims=True)

    order = (2, 1, 3, 0)

    def products(ru, side):
        rows = jnp.concatenate([actT[dp_of(ru, rv)] for rv in range(4)], axis=0)
        res = tn(rows, del2[:, side]).astype(BF)
        for rv in range(4):
            part[ru, rv, :, side] = res[rv * 128 : (rv + 1) * 128]

    left, right = pl.ds(0, LEFT), pl.ds(LEFT, RIGHT)
    one_a, one_b, two_a, two_b = [None] * 4, [None] * 4, [None] * 4, [None] * 4
    first, last = (2, 1), (3, 0)

    def step_one(side, rvs):
        for rv in rvs:
            if side == 0:
                one_a[rv] = send(part.at[2, rv, :, left], r1a.at[rv], u1)
            else:
                one_b[rv] = send(part.at[2, rv, :, right], r1b.at[rv], u3)

    def raw(side, rvs):
        for rv in rvs:
            if side == 0:
                two_a[rv] = [send(part.at[1, rv, :, left], r2a.at[rv, :, left], u1)]
            else:
                two_b[rv] = [send(part.at[3, rv, :, right], r2b.at[rv, :, right], u3)]

    def merge(rvs):
        for rv in rvs:
            one_a[rv].wait_recv()
            part[3, rv, :, left] = (part[3, rv, :, left].astype(F32) + r1a[rv].astype(F32)).astype(BF)
            two_b[rv].append(send(part.at[3, rv, :, left], r2b.at[rv, :, left], u3))
            one_b[rv].wait_recv()
            part[1, rv, :, right] = (part[1, rv, :, right].astype(F32) + r1b[rv].astype(F32)).astype(BF)
            two_a[rv].append(send(part.at[1, rv, :, right], r2a.at[rv, :, right], u1))

    products(2, right)
    step_one(1, order)
    products(2, left)
    step_one(0, order)
    products(1, left)
    raw(0, first)

    featT[...] = jnp.transpose(feat[...])

    @pl.loop(0, H // C5)
    def _(n):
        cols = chunk(n, C5)
        back = nt(del2[...], wmid[cols, :])
        d = back * sl1[:, cols].astype(F32)
        stats[0:1, cols] = jnp.sum(d, axis=0, keepdims=True)
        res = tn(featT[...], d.astype(BF)).astype(BF)
        for i in range(16):
            slot = jnp.where(core == 0, (i // 4 ^ y) * 4 + (i % 4 ^ z), (i % 4 ^ z) * 4 + (i // 4 ^ y))
            gp[slot, :, cols] = res[i * 16 : (i + 1) * 16]

    for i in range(16):
        slot = jnp.where(core == 0, (i // 4 ^ y) * 4 + (i % 4 ^ z), (i % 4 ^ z) * 4 + (i // 4 ^ y))
        tile = jnp.concatenate([stats[:, i * 128 : (i + 1) * 128], jnp.zeros((8, 128), F32)], axis=0)
        gp[slot, :, pl.ds(H, 128)] = tile.astype(BF)

    gl, gr = pl.ds(0, GL), pl.ds(GL, GR)
    g_one_a = send(gp.at[pl.ds(8, 4), :, gl], g1a, u1)
    g_one_b = send(gp.at[pl.ds(8, 4), :, gr], g1b, u3)
    g_two_a = [send(gp.at[pl.ds(4, 4), :, gl], g2a.at[:, :, gl], u1)]
    g_two_b = [send(gp.at[pl.ds(12, 4), :, gr], g2b.at[:, :, gr], u3)]

    got_q.wait_recv()
    mo[...] = jnp.minimum(mo[...], qr[...])
    got_sib = send(mo, ms, sib)

    products(3, right)
    raw(1, first)
    products(1, right)
    products(3, left)
    g_one_a.wait_recv()
    gp[12:16, :, gl] = (gp[12:16, :, gl].astype(F32) + g1a[...].astype(F32)).astype(BF)
    g_two_b.append(send(gp.at[pl.ds(12, 4), :, gl], g2b.at[:, :, gl], u3))
    g_one_b.wait_recv()
    gp[4:8, :, gr] = (gp[4:8, :, gr].astype(F32) + g1b[...].astype(F32)).astype(BF)
    g_two_a.append(send(gp.at[pl.ds(4, 4), :, gr], g2a.at[:, :, gr], u1))
    merge(first)
    raw(0, last)
    raw(1, last)
    merge(last)
    got_sib.wait_recv()
    mm[...] = jnp.minimum(mo[...], ms[...])
    got_x = [send(mm, mx.at[k], xs[k]) for k in range(3)]
    products(0, left)
    products(0, right)

    sides = (left, right)

    def ring_sum(rv, half):
        two_a[rv][half].wait_recv()
        two_b[rv][1 - half].wait_recv()
        at = sides[half]
        return part[0, rv, :, at].astype(F32) + r2a[rv, :, at].astype(F32) + r2b[rv, :, at].astype(F32)

    three = {}
    for rv, slot in ((2, 1), (1, 0)):
        for half, at in enumerate(sides):
            part[0, rv, :, at] = ring_sum(rv, half).astype(BF)
            three[slot, half] = send(part.at[0, rv, :, at], r3.at[slot, :, at], v1)
    for copy in (*g_two_a, *g_two_b):
        copy.wait_recv()
    gp[0:4] = (gp[0:4].astype(F32) + g2a[...].astype(F32) + g2b[...].astype(F32)).astype(BF)
    g_three = send(gp.at[pl.ds(1, 2)], g3, v1)

    four = []
    for half, at in enumerate(sides):
        total = ring_sum(3, half)
        three[1, half].wait_recv()
        part[0, 3, :, at] = (total + r3[1, :, at].astype(F32)).astype(BF)
        four.append(send(part.at[0, 3, :, at], mid_out.at[head, :, at], v3))

    g_three.wait_recv()
    gp[3] = (gp[3].astype(F32) + g3[1].astype(F32)).astype(BF)
    g_four = send(gp.at[3], gin_out.at[head], v3)
    gp[0] = (gp[0].astype(F32) + g3[0].astype(F32)).astype(BF)
    own_gin = pltpu.make_async_copy(gp.at[0], gin_out.at[head], osem.at[2])
    own_gin.start()

    own_mid = []
    for half, at in enumerate(sides):
        total = ring_sum(0, half)
        three[0, half].wait_recv()
        part[0, 0, :, at] = (total + r3[0, :, at].astype(F32)).astype(BF)
        copy = pltpu.make_async_copy(part.at[0, 0, :, at], mid_out.at[head, :, at], osem.at[half])
        copy.start()
        own_mid.append(copy)

    for copy in got_x:
        copy.wait_recv()
    q_min = jnp.minimum(jnp.minimum(mm[...], mx[0]), jnp.minimum(mx[1], mx[2]))
    gap = q_min[0:1] - vnow[...].reshape(1, ROWS)
    vg_out[...] = -2.0 * jnp.where(gap < 0.0, 0.3, 0.7) * gap

    for copy in own_mid:
        copy.wait()
    own_gin.wait()
    for copy in four:
        copy.wait_recv()
    g_four.wait_recv()
    for copy in copies:
        copy.wait_send()


def finish(vg, mid, gin, vg_out, din, dmid, dbias, dout):
    vg_out[...] = vg[...].reshape(ROWS)
    for h in range(2):
        dmid[:, h, :] = mid[h].astype(F32)
        din[:, h, :] = gin[h, :, :H].astype(F32)
        rest = gin[h, :, H:].astype(F32)
        dbias[0, h : h + 1, :] = rest[0:1]
        dbias[1, h : h + 1, :] = rest[1:2]
        dout[h : h + 1, :] = rest[2:3]


def per_device(features, reward, done, value_next, value_now, w_in, w_mid, biases, w_out):
    vm = pl.BlockSpec(memory_space=pltpu.VMEM)
    hbm = pl.BlockSpec(memory_space=pl.ANY)
    line = (1, ROWS)
    vg, mid, gin = pl.pallas_call(
        kernel,
        out_shape=(
            jax.ShapeDtypeStruct(line, F32),
            jax.ShapeDtypeStruct((2, 128, H), BF),
            jax.ShapeDtypeStruct((2, 16, GW), BF),
        ),
        in_specs=[hbm] * 9,
        out_specs=(vm, hbm, hbm),
        scratch_shapes=[
            pltpu.VMEM((R2, IN), BF),
            pltpu.VMEM((IN, H), BF),
            pltpu.VMEM((H, H), BF),
            pltpu.VMEM((R2, H), BF),
            pltpu.VMEM((R2, H), BF),
            pltpu.VMEM((R2, H), BF),
            pltpu.VMEM((R2, H), BF),
            pltpu.VMEM((R2, H), BF),
            pltpu.VMEM((R2, 128), F32),
            pltpu.VMEM((R2, 128), F32),
            pltpu.VMEM((8, H), F32),
            pltpu.VMEM((4, 4, 128, H), BF),
            pltpu.VMEM((16, 128, R2), BF),
            pltpu.VMEM((IN, R2), BF),
            pltpu.VMEM((4, 128, LEFT), BF),
            pltpu.VMEM((4, 128, RIGHT), BF),
            pltpu.VMEM((4, 128, H), BF),
            pltpu.VMEM((4, 128, H), BF),
            pltpu.VMEM((2, 128, H), BF),
            pltpu.VMEM((16, 16, GW), BF),
            pltpu.VMEM((4, 16, GL), BF),
            pltpu.VMEM((4, 16, GR), BF),
            pltpu.VMEM((4, 16, GW), BF),
            pltpu.VMEM((4, 16, GW), BF),
            pltpu.VMEM((2, 16, GW), BF),
            pltpu.VMEM((ROWS,), F32),
            pltpu.VMEM((ROWS,), jnp.int32),
            pltpu.VMEM((ROWS,), F32),
            pltpu.VMEM((ROWS,), F32),
            pltpu.VMEM((2, 2, H), F32),
            pltpu.VMEM((2, H), BF),
            *[pltpu.VMEM((8, ROWS), F32)] * 7,
            pltpu.VMEM((3, 8, ROWS), F32),
            pltpu.SemaphoreType.DMA((8,)),
            pltpu.SemaphoreType.DMA((NC,)),
            pltpu.SemaphoreType.DMA((3,)),
            pltpu.SemaphoreType.DMA((56,)),
            pltpu.SemaphoreType.DMA((56,)),
        ],
        compiler_params=pltpu.CompilerParams(
            collective_id=0, has_side_effects=True, vmem_limit_bytes=67_000_000
        ),
    )(
        features, reward, done, value_next, value_now, w_in, w_mid, biases, w_out,
    )
    return pl.pallas_call(
        finish,
        out_shape=(
            jax.ShapeDtypeStruct((ROWS,), F32),
            jax.ShapeDtypeStruct((16, 2, H), F32),
            jax.ShapeDtypeStruct((128, 2, H), F32),
            jax.ShapeDtypeStruct((2, 2, 128), F32),
            jax.ShapeDtypeStruct((2, 128), F32),
        ),
        in_specs=[vm, vm, vm],
        out_specs=(vm,) * 5,
    )(vg, mid, gin)


def solution(mesh):
    in_specs = (
        P("dp", None), P("dp"), P("dp"), P("dp"), P("dp"),
        P("ens", None, None), P("ens", None, None), P(None, "ens", None), P("ens", None),
    )
    out_specs = (
        P("dp"), P("dp", "ens", None), P("dp", "ens", None), P(None, "ens", "dp"), P("ens", "dp"),
    )
    return jax.shard_map(
        per_device, mesh=mesh, in_specs=in_specs, out_specs=out_specs, check_vma=False
    )
```

```python
import jax
import jax.numpy as jnp
from jax import lax
from jax.experimental import pallas as pl
from jax.experimental.pallas import tpu as pltpu
from jax.sharding import PartitionSpec as P

MESH = pl.DeviceIdType.MESH
BF = jnp.bfloat16
F32 = jnp.float32
ROWS = 384
IN = 256
H = 2048
R2 = 2 * ROWS
C = 256
NC = H // C
C1 = 512
C2 = 512
C3 = 512
C5 = 512
GW = H + 128
LEFT = 768
RIGHT = H - LEFT
GL = 896
GR = GW - GL


def tn(a, b, **kw):
    return lax.dot_general(a, b, (((1,), (0,)), ((), ())), preferred_element_type=F32, **kw)


def nt(a, b, **kw):
    return lax.dot_general(a, b, (((1,), (1,)), ((), ())), preferred_element_type=F32, **kw)


def chunk(n, width=C):
    return pl.ds(pl.multiple_of(n * width, width), width)


def kernel(
    feat_hbm, reward_hbm, done_hbm, vnext_hbm, vnow_hbm, win_hbm, wmid_hbm, biases_hbm, wout_hbm,
    vg_out, mid_out, gin_out,
    feat, win, wmid, act1, sl1, act2, sl2, del2, accq, eb, stats, part, actT, featT,
    r1a, r1b, r2a, r2b, r3, gp, g1a, g1b, g2a, g2b, g3,
    reward, done, vnext, vnow, biases, wout, tgt, tgtm, qm, qr, mo, ms, mm, mx,
    lsem, wsem, osem, ssem, rsem,
):
    ens = lax.axis_index("ens")
    dp = lax.axis_index("dp")
    core = lax.rem(ens, 2)
    xpos = lax.div(ens, 2)
    y = lax.div(dp, 4)
    z = lax.rem(dp, 4)
    u = jnp.where(core == 0, y, z)
    v = jnp.where(core == 0, z, y)
    su = 4 - 3 * core
    sv = 1 + 3 * core
    head = lax.div(v, 2)

    def dp_of(ru, rv):
        return (u ^ ru) * su + (v ^ rv) * sv

    def dev(ru, rv):
        return (ens, dp_of(ru, rv))

    u1, u3, v1, v3 = dev(1, 0), dev(3, 0), dev(0, 1), dev(0, 3)
    sib = (ens ^ 1, dp)
    xs = [((xpos ^ k) * 2 + core, dp) for k in (1, 2, 3)]

    barrier = pltpu.get_barrier_semaphore()
    partners = [u1, u3, v1, v3, sib, *xs]
    for p in partners:
        pl.semaphore_signal(barrier, inc=1, device_id=p, device_id_type=MESH)

    loads = [
        pltpu.make_async_copy(feat_hbm, feat.at[pl.ds(0, ROWS)], lsem.at[0]),
        pltpu.make_async_copy(win_hbm.at[head], win, lsem.at[1]),
    ]
    for n in range(NC):
        loads.append(
            pltpu.make_async_copy(
                wmid_hbm.at[head, pl.ds(n * C, C)], wmid.at[pl.ds(n * C, C)], wsem.at[n]
            )
        )
    for copy in loads[:2]:
        copy.start()

    small = [
        pltpu.make_async_copy(src, dst, lsem.at[2 + i])
        for i, (src, dst) in enumerate(
            (
                (biases_hbm, biases), (wout_hbm, wout), (reward_hbm, reward), (done_hbm, done),
                (vnext_hbm, vnext), (vnow_hbm, vnow),
            )
        )
    ]
    for copy in small:
        copy.start()

    for copy in loads[2:]:
        copy.start()

    for copy in small:
        copy.wait()
    target = reward[...] + 0.99 * (1.0 - done[...].astype(F32)) * vnext[...]
    tgt[...] = jnp.broadcast_to(target.reshape(1, ROWS), (8, ROWS))
    loads[0].wait()
    loads[1].wait()

    wo = wout[...].astype(F32)
    wo = jnp.where(head == 0, wo[0:1], wo[1:2])
    b_all = biases[...]
    b_one = jnp.where(head == 0, b_all[0, 0:1], b_all[0, 1:2])
    b_two = jnp.where(head == 0, b_all[1, 0:1], b_all[1, 1:2])
    stats[...] = jnp.zeros_like(stats)
    stats[0:1, :] = b_one
    stats[1:2, :] = b_two
    stats[2:3, :] = wo

    def silu_both(val):
        s = 0.5 * jnp.tanh(0.5 * val) + 0.5
        act = val * s
        return act, s + act * (1.0 - s)

    accq[...] = jnp.zeros_like(accq)

    def layer_one(p):
        rows = pl.ds(p * ROWS, ROWS)

        @pl.loop(0, H // C1)
        def _(n):
            cols = chunk(n, C1)
            val = tn(feat[rows, :], win[:, cols]) + stats[0:1, cols]
            act, slope = silu_both(val)
            act1[rows, cols] = act.astype(BF)
            sl1[rows, cols] = slope.astype(BF)

    pl.semaphore_wait(barrier, len(partners))

    copies = []

    def send(src, dst, to):
        i = len(copies)
        copy = pltpu.make_async_remote_copy(
            src_ref=src, dst_ref=dst, send_sem=ssem.at[i], recv_sem=rsem.at[i],
            device_id=to, device_id_type=MESH,
        )
        copies.append(copy)
        copy.start()
        return copy

    got_feat = send(feat.at[pl.ds(0, ROWS)], feat.at[pl.ds(ROWS, ROWS)], v3)
    got_tgt = send(tgt, tgtm, v3)
    def layer_two(p):
        rows = pl.ds(p * ROWS, ROWS)

        @pl.loop(0, H // C2)
        def _(n):
            cols = chunk(n, C2)
            if p == 1:
                for i in range(C2 // 128):
                    d = n * (C2 // 128) + i
                    actT[d] = jnp.transpose(act1[:, chunk(d, 128)])
            val = tn(act1[rows, :], wmid[:, cols]) + stats[1:2, cols]
            act, slope = silu_both(val)
            wrow = stats[2:3, cols]
            prod = act * wrow
            accq[rows, :] += sum(prod[:, i * 128 : (i + 1) * 128] for i in range(C2 // 128))
            act2[rows, cols] = act.astype(BF)
            sl2[rows, cols] = (slope * wrow).astype(BF)

    layer_one(0)
    for copy in loads[2:]:
        copy.wait()
    layer_two(0)
    got_feat.wait_recv()
    layer_one(1)
    layer_two(1)

    q = nt(jnp.ones((8, 128), F32), accq[...], precision=lax.Precision.HIGHEST)
    got_tgt.wait_recv()
    qm[...] = q[:, ROWS:]
    mo[...] = q[:, :ROWS]
    got_q = send(qm, qr, v3)
    err = q - jnp.concatenate([tgt[...], tgtm[...]], axis=1)
    eb[...] = jnp.transpose(jnp.broadcast_to(err[0:1], (128, R2)))
    stats[...] = jnp.zeros_like(stats)

    @pl.loop(0, H // C3)
    def _(n):
        cols = chunk(n, C3)
        e = jnp.concatenate([eb[...]] * (C3 // 128), axis=1)
        d = e * sl2[:, cols].astype(F32)
        del2[:, cols] = d.astype(BF)
        stats[1:2, cols] = jnp.sum(d, axis=0, keepdims=True)
        stats[2:3, cols] = jnp.sum(e * act2[:, cols].astype(F32), axis=0, keepdims=True)

    order = (2, 1, 3, 0)

    def products(ru, side):
        rows = jnp.concatenate([actT[dp_of(ru, rv)] for rv in range(4)], axis=0)
        res = tn(rows, del2[:, side]).astype(BF)
        for rv in range(4):
            part[ru, rv, :, side] = res[rv * 128 : (rv + 1) * 128]

    left, right = pl.ds(0, LEFT), pl.ds(LEFT, RIGHT)
    one_a, one_b, two_a, two_b = [None] * 4, [None] * 4, [None] * 4, [None] * 4
    first, last = (2, 1), (3, 0)

    def step_one(side, rvs):
        for rv in rvs:
            if side == 0:
                one_a[rv] = send(part.at[2, rv, :, left], r1a.at[rv], u1)
            else:
                one_b[rv] = send(part.at[2, rv, :, right], r1b.at[rv], u3)

    def raw(side, rvs):
        for rv in rvs:
            if side == 0:
                two_a[rv] = [send(part.at[1, rv, :, left], r2a.at[rv, :, left], u1)]
            else:
                two_b[rv] = [send(part.at[3, rv, :, right], r2b.at[rv, :, right], u3)]

    def merge(rvs):
        for rv in rvs:
            one_a[rv].wait_recv()
            part[3, rv, :, left] = (part[3, rv, :, left].astype(F32) + r1a[rv].astype(F32)).astype(BF)
            two_b[rv].append(send(part.at[3, rv, :, left], r2b.at[rv, :, left], u3))
            one_b[rv].wait_recv()
            part[1, rv, :, right] = (part[1, rv, :, right].astype(F32) + r1b[rv].astype(F32)).astype(BF)
            two_a[rv].append(send(part.at[1, rv, :, right], r2a.at[rv, :, right], u1))

    products(2, right)
    step_one(1, order)
    products(2, left)
    step_one(0, order)
    products(1, left)
    raw(0, first)

    featT[...] = jnp.transpose(feat[...])

    @pl.loop(0, H // C5)
    def _(n):
        cols = chunk(n, C5)
        back = nt(del2[...], wmid[cols, :])
        d = back * sl1[:, cols].astype(F32)
        stats[0:1, cols] = jnp.sum(d, axis=0, keepdims=True)
        res = tn(featT[...], d.astype(BF)).astype(BF)
        for i in range(16):
            slot = jnp.where(core == 0, (i // 4 ^ y) * 4 + (i % 4 ^ z), (i % 4 ^ z) * 4 + (i // 4 ^ y))
            gp[slot, :, cols] = res[i * 16 : (i + 1) * 16]

    for i in range(16):
        slot = jnp.where(core == 0, (i // 4 ^ y) * 4 + (i % 4 ^ z), (i % 4 ^ z) * 4 + (i // 4 ^ y))
        tile = jnp.concatenate([stats[:, i * 128 : (i + 1) * 128], jnp.zeros((8, 128), F32)], axis=0)
        gp[slot, :, pl.ds(H, 128)] = tile.astype(BF)

    gl, gr = pl.ds(0, GL), pl.ds(GL, GR)
    g_one_a = send(gp.at[pl.ds(8, 4), :, gl], g1a, u1)
    g_one_b = send(gp.at[pl.ds(8, 4), :, gr], g1b, u3)
    g_two_a = [send(gp.at[pl.ds(4, 4), :, gl], g2a.at[:, :, gl], u1)]
    g_two_b = [send(gp.at[pl.ds(12, 4), :, gr], g2b.at[:, :, gr], u3)]

    got_q.wait_recv()
    mo[...] = jnp.minimum(mo[...], qr[...])
    got_sib = send(mo, ms, sib)

    products(3, right)
    raw(1, first)
    products(1, right)
    products(3, left)
    g_one_a.wait_recv()
    gp[12:16, :, gl] = (gp[12:16, :, gl].astype(F32) + g1a[...].astype(F32)).astype(BF)
    g_two_b.append(send(gp.at[pl.ds(12, 4), :, gl], g2b.at[:, :, gl], u3))
    g_one_b.wait_recv()
    gp[4:8, :, gr] = (gp[4:8, :, gr].astype(F32) + g1b[...].astype(F32)).astype(BF)
    g_two_a.append(send(gp.at[pl.ds(4, 4), :, gr], g2a.at[:, :, gr], u1))
    merge(first)
    raw(0, last)
    raw(1, last)
    merge(last)
    got_sib.wait_recv()
    mm[...] = jnp.minimum(mo[...], ms[...])
    got_x = [send(mm, mx.at[k], xs[k]) for k in range(3)]
    products(0, left)
    products(0, right)

    sides = (left, right)

    def ring_sum(rv, half):
        two_a[rv][half].wait_recv()
        two_b[rv][1 - half].wait_recv()
        at = sides[half]
        return part[0, rv, :, at].astype(F32) + r2a[rv, :, at].astype(F32) + r2b[rv, :, at].astype(F32)

    three = {}
    for rv, slot in ((2, 1), (1, 0)):
        for half, at in enumerate(sides):
            part[0, rv, :, at] = ring_sum(rv, half).astype(BF)
            three[slot, half] = send(part.at[0, rv, :, at], r3.at[slot, :, at], v1)
    for copy in (*g_two_a, *g_two_b):
        copy.wait_recv()
    gp[0:4] = (gp[0:4].astype(F32) + g2a[...].astype(F32) + g2b[...].astype(F32)).astype(BF)
    g_three = send(gp.at[pl.ds(1, 2)], g3, v1)

    four = []
    for half, at in enumerate(sides):
        total = ring_sum(3, half)
        three[1, half].wait_recv()
        part[0, 3, :, at] = (total + r3[1, :, at].astype(F32)).astype(BF)
        four.append(send(part.at[0, 3, :, at], mid_out.at[head, :, at], v3))

    g_three.wait_recv()
    gp[3] = (gp[3].astype(F32) + g3[1].astype(F32)).astype(BF)
    g_four = send(gp.at[3], gin_out.at[head], v3)
    gp[0] = (gp[0].astype(F32) + g3[0].astype(F32)).astype(BF)
    own_gin = pltpu.make_async_copy(gp.at[0], gin_out.at[head], osem.at[2])
    own_gin.start()

    own_mid = []
    for half, at in enumerate(sides):
        total = ring_sum(0, half)
        three[0, half].wait_recv()
        part[0, 0, :, at] = (total + r3[0, :, at].astype(F32)).astype(BF)
        copy = pltpu.make_async_copy(part.at[0, 0, :, at], mid_out.at[head, :, at], osem.at[half])
        copy.start()
        own_mid.append(copy)

    for copy in got_x:
        copy.wait_recv()
    q_min = jnp.minimum(jnp.minimum(mm[...], mx[0]), jnp.minimum(mx[1], mx[2]))
    gap = q_min[0:1] - vnow[...].reshape(1, ROWS)
    vg_out[...] = -2.0 * jnp.where(gap < 0.0, 0.3, 0.7) * gap

    for copy in own_mid:
        copy.wait()
    own_gin.wait()
    for copy in four:
        copy.wait_recv()
    g_four.wait_recv()
    for copy in copies:
        copy.wait_send()


def finish(vg, mid, gin, vg_out, din, dmid, dbias, dout):
    vg_out[...] = vg[...].reshape(ROWS)
    for h in range(2):
        dmid[:, h, :] = mid[h].astype(F32)
        din[:, h, :] = gin[h, :, :H].astype(F32)
        rest = gin[h, :, H:].astype(F32)
        dbias[0, h : h + 1, :] = rest[0:1]
        dbias[1, h : h + 1, :] = rest[1:2]
        dout[h : h + 1, :] = rest[2:3]


def per_device(features, reward, done, value_next, value_now, w_in, w_mid, biases, w_out):
    vm = pl.BlockSpec(memory_space=pltpu.VMEM)
    hbm = pl.BlockSpec(memory_space=pl.ANY)
    line = (1, ROWS)
    vg, mid, gin = pl.pallas_call(
        kernel,
        out_shape=(
            jax.ShapeDtypeStruct(line, F32),
            jax.ShapeDtypeStruct((2, 128, H), BF),
            jax.ShapeDtypeStruct((2, 16, GW), BF),
        ),
        in_specs=[hbm] * 9,
        out_specs=(vm, hbm, hbm),
        scratch_shapes=[
            pltpu.VMEM((R2, IN), BF),
            pltpu.VMEM((IN, H), BF),
            pltpu.VMEM((H, H), BF),
            pltpu.VMEM((R2, H), BF),
            pltpu.VMEM((R2, H), BF),
            pltpu.VMEM((R2, H), BF),
            pltpu.VMEM((R2, H), BF),
            pltpu.VMEM((R2, H), BF),
            pltpu.VMEM((R2, 128), F32),
            pltpu.VMEM((R2, 128), F32),
            pltpu.VMEM((8, H), F32),
            pltpu.VMEM((4, 4, 128, H), BF),
            pltpu.VMEM((16, 128, R2), BF),
            pltpu.VMEM((IN, R2), BF),
            pltpu.VMEM((4, 128, LEFT), BF),
            pltpu.VMEM((4, 128, RIGHT), BF),
            pltpu.VMEM((4, 128, H), BF),
            pltpu.VMEM((4, 128, H), BF),
            pltpu.VMEM((2, 128, H), BF),
            pltpu.VMEM((16, 16, GW), BF),
            pltpu.VMEM((4, 16, GL), BF),
            pltpu.VMEM((4, 16, GR), BF),
            pltpu.VMEM((4, 16, GW), BF),
            pltpu.VMEM((4, 16, GW), BF),
            pltpu.VMEM((2, 16, GW), BF),
            pltpu.VMEM((ROWS,), F32),
            pltpu.VMEM((ROWS,), jnp.int32),
            pltpu.VMEM((ROWS,), F32),
            pltpu.VMEM((ROWS,), F32),
            pltpu.VMEM((2, 2, H), F32),
            pltpu.VMEM((2, H), BF),
            *[pltpu.VMEM((8, ROWS), F32)] * 7,
            pltpu.VMEM((3, 8, ROWS), F32),
            pltpu.SemaphoreType.DMA((8,)),
            pltpu.SemaphoreType.DMA((NC,)),
            pltpu.SemaphoreType.DMA((3,)),
            pltpu.SemaphoreType.DMA((56,)),
            pltpu.SemaphoreType.DMA((56,)),
        ],
        compiler_params=pltpu.CompilerParams(
            collective_id=0, has_side_effects=True, vmem_limit_bytes=67_000_000
        ),
    )(
        features, reward, done, value_next, value_now, w_in, w_mid, biases, w_out,
    )
    return pl.pallas_call(
        finish,
        out_shape=(
            jax.ShapeDtypeStruct((ROWS,), F32),
            jax.ShapeDtypeStruct((16, 2, H), F32),
            jax.ShapeDtypeStruct((128, 2, H), F32),
            jax.ShapeDtypeStruct((2, 2, 128), F32),
            jax.ShapeDtypeStruct((2, 128), F32),
        ),
        in_specs=[vm, vm, vm],
        out_specs=(vm,) * 5,
    )(vg, mid, gin)


def solution(mesh):
    in_specs = (
        P("dp", None), P("dp"), P("dp"), P("dp"), P("dp"),
        P("ens", None, None), P("ens", None, None), P(None, "ens", None), P("ens", None),
    )
    out_specs = (
        P("dp"), P("dp", "ens", None), P("dp", "ens", None), P(None, "ens", "dp"), P("ens", "dp"),
    )
    return jax.shard_map(
        per_device, mesh=mesh, in_specs=in_specs, out_specs=out_specs, check_vma=False
    )
```
